32 devices in a mesh: dp: 4 (over z), seq: 8 (over y, x, core).
Axes of the slice: x: 2, y: 2, z: 4, core: 2. Of those that a mesh axis runs over, the one named last changes fastest.
Arguments:
- queries: bfloat16 [4, 2048, 512], P('dp', 'seq'), may hold values from -0.890625 to 0.890625
- keys: bfloat16 [4, 2048, 512], P('dp', 'seq'), may hold values from -0.890625 to 0.890625
- values: bfloat16 [4, 2048, 512], P('dp', 'seq'), may hold values from -6 to 6
- level_weights: float32 [4, 6, 4, 2048], P('dp', None, None, 'seq'), may hold values from 0.25 to 4
- proj: bfloat16 [512, 2048], P(None, 'seq'), may hold values from -0.25 to 0.25
- out_grad: bfloat16 [4, 2048, 2048], P('dp', 'seq'), may hold values from -0.59765625 to 0.59765625
Outputs:
- attended_out: bfloat16 [4, 2048, 2048], P('dp', 'seq')
- grad_queries: bfloat16 [4, 2048, 512], P('dp', 'seq')
- grad_keys: bfloat16 [4, 2048, 512], P('dp', 'seq')
- grad_values: bfloat16 [4, 2048, 512], P('dp', 'seq')
- grad_levels: float32 [4, 6, 4, 2048], P('dp', None, None, 'seq')
- grad_proj: float32 [512, 2048], P(None, 'seq')
The draws below stay inside these ranges and needn't reach their ends.
All inputs are finite; a program needn't handle non-finite values.
Results may differ from the reference program's by a relative error of at most 0.0064.
Values may be sent and summed in bfloat16 or wider, within the bound.
No kernel may reach another device: no remote copies, remote signals or barrier semaphores. Data moves between devices by JAX's collectives and lax.ppermute only.
A program may use at most 64 MiB of HBM per device.

```python
import math
import jax
import jax.numpy as jnp
from jax import lax

HEADS = 4
HEAD_DIM = 128
DOUT = 2048
LOCAL_BITS = 2
STRETCH = 64
WIDTH = 512
TOK_DEV = 256
DEV_BITS = 3
LEVELS = 6
TOKENS = 2048
BATCH = 4
N_SEQ = 8


def with_spikes(array, rng, source, target, shards_of, factor):
    def block_of(dim):
        return (jnp.arange(array.shape[dim]) // (array.shape[dim] // shards_of)).reshape((-1,) + (1,) * (array.ndim - 1 - dim))

    near = jax.random.permutation(rng, shards_of)[block_of(target)]
    far = (block_of(target) + shards_of // 2) % shards_of
    return jnp.where((block_of(source) == near) | (block_of(source) == far), factor * array, array)


def levels(rng, extent, cuts, low, high):
    def one(axis_at, shards_of):
        heights = jax.random.uniform(jax.random.fold_in(jax.random.fold_in(rng, 6), axis_at), (shards_of,), jnp.float32, low / len(cuts), high / len(cuts))
        return jnp.repeat(jnp.exp(heights), extent[axis_at] // shards_of).reshape((-1,) + (1,) * (len(extent) - axis_at - 1))

    loudness = one(*cuts[0])
    for cut in cuts[1:]:
        loudness = loudness * one(*cut)
    return loudness


def noise(stream_key, dims, spread, bound, split=(), dtype=jnp.bfloat16):
    factor_of = levels(stream_key, dims, split, -0.22, 0.18) if split else 1.0
    array = jax.random.normal(stream_key, dims, jnp.float32) * spread * factor_of
    return jnp.minimum(jnp.maximum(array, -bound), bound).astype(dtype)


def gaussian_with(own_key, shape, deviation, most, split, heavy, dtype=jnp.bfloat16):
    result = deviation * jax.random.normal(own_key, shape, jnp.float32)
    if split:
        result = result * levels(own_key, shape, split, -0.22, 0.18)
    return jnp.clip(with_spikes(result, jax.random.fold_in(own_key, 3), *heavy), -most, most).astype(dtype)


def setup_inputs(seed: int = 0) -> dict:
    streams_of = jax.random.split(jax.random.key(seed), 7)
    queries = noise(streams_of[0], (BATCH, TOKENS, WIDTH), (1.0 / TOKENS ** 0.25), 0.890625, ((0, 4), (1, 8)))
    keys = noise(streams_of[1], (BATCH, TOKENS, WIDTH), (1.0 / TOKENS ** 0.25), 0.890625, ((0, 4), (1, 8)))
    values = noise(streams_of[2], (BATCH, TOKENS, WIDTH), 1.0, 6.0, ((0, 4), (1, 8)))
    level_weights = jnp.clip(jnp.exp(math.log(4.0) - 2.7725887 * jax.random.uniform(streams_of[3], (BATCH, LEVELS, HEADS, TOKENS), jnp.float32) ** levels(streams_of[3], (BATCH, LEVELS, HEADS, TOKENS), ((0, 4), (3, 8)), -0.2, 0.2)), 0.25, 4.0)
    proj = noise(streams_of[4], (WIDTH, DOUT), WIDTH ** -0.5, 0.25, ((1, 8),))
    out_grad = gaussian_with(streams_of[5], (BATCH, TOKENS, DOUT), 0.1, 0.59765625, ((0, 4), (1, 8)), (1, 2, 8, 2.0))
    return {"queries": queries, "keys": keys, "values": values, "level_weights": level_weights, "proj": proj, "out_grad": out_grad}


def level_table(length, stretch, local_bits):
    place = lax.iota(jnp.int32, length)
    blocks = place // stretch
    apart = jnp.bitwise_xor(blocks[:, None], blocks[None, :])
    table = jnp.zeros((length, length), jnp.int32)
    for bit in range(local_bits):
        table = table + (apart >= (1 << bit)).astype(jnp.int32)
    causal = place[:, None] >= place[None, :]
    return table, causal


def local_weights(lam, table, causal, local_bits):
    weights = jnp.zeros((lam.shape[1], table.shape[0], table.shape[1]), jnp.float32)
    for level in range(local_bits + 1):
        weights = weights + jnp.where(table[None] == level, lam[level][:, :, None], jnp.float32(0))
    return jnp.where(causal[None], weights, jnp.float32(0))


def bucket_masks(count, bits):
    spans = lax.iota(jnp.int32, count)
    rows = []
    for bit in range(bits):
        upper = jnp.right_shift(spans, bit + 1)
        marked = jnp.bitwise_and(jnp.right_shift(spans, bit), 1)
        inside = (upper[:, None] == upper[None, :]) & (marked[:, None] == 1) & (marked[None, :] == 0)
        rows.append(inside.astype(jnp.float32))
    return jnp.stack(rows)


def span_forward(query, key, value, lam, states):
    scale = HEAD_DIM ** -0.5
    table, causal = level_table(TOK_DEV, STRETCH, LOCAL_BITS)
    qf = query.astype(jnp.float32)
    kf = key.astype(jnp.float32)
    vf = value.astype(jnp.float32)
    scores = jnp.einsum('thd,shd->hts', qf, kf)
    weights = local_weights(lam, table, causal, LOCAL_BITS)
    probs = (scale * weights * scores).astype(jnp.bfloat16)
    total = jnp.einsum('hts,shd->thd', probs.astype(jnp.float32), vf)
    cross = jnp.zeros_like(total)
    mapped = []
    for bit in range(DEV_BITS):
        image = jnp.einsum('thi,hij->thj', qf, states[bit].astype(jnp.float32))
        mapped.append(image)
        cross = cross + lam[LOCAL_BITS + 1 + bit].T[:, :, None] * image
    attended = (total + scale * cross).astype(jnp.bfloat16)
    return attended, scores, weights, probs, mapped, table, causal


def span_backward(query, key, value, lam, states, grad_att):
    scale = HEAD_DIM ** -0.5
    attended, scores, weights, probs, mapped, table, causal = span_forward(query, key, value, lam, states)
    qf = query.astype(jnp.float32)
    kf = key.astype(jnp.float32)
    vf = value.astype(jnp.float32)
    gf = grad_att.astype(jnp.float32)
    dprob = jnp.einsum('thd,shd->hts', gf, vf)
    product = jnp.where(causal[None], scale * scores * dprob, jnp.float32(0))
    grads = [jnp.sum(jnp.where(table[None] == level, product, jnp.float32(0)), axis=2) for level in range(LOCAL_BITS + 1)]
    dscore = (scale * weights * dprob).astype(jnp.bfloat16)
    dq = jnp.einsum('hts,shd->thd', dscore.astype(jnp.float32), kf)
    dk = jnp.einsum('hts,thd->shd', dscore.astype(jnp.float32), qf)
    dv = jnp.einsum('hts,thd->shd', probs.astype(jnp.float32), gf)
    updates = []
    for bit in range(DEV_BITS):
        grads.append(scale * jnp.sum(gf * mapped[bit], axis=2).T)
        weighted = (scale * lam[LOCAL_BITS + 1 + bit].T[:, :, None] * gf).astype(jnp.bfloat16)
        updates.append(jnp.einsum('thi,thj->hij', qf, weighted.astype(jnp.float32)))
        dq = dq + jnp.einsum('thj,hij->thi', weighted.astype(jnp.float32), states[bit].astype(jnp.float32))
    return dq, dk, dv, jnp.stack(grads), jnp.stack(updates)


def one_sequence(query, key, value, lam, grad_out, proj):
    shape = (N_SEQ, TOK_DEV, HEADS, HEAD_DIM)
    qs = query.reshape(shape)
    ks = key.reshape(shape)
    vs = value.reshape(shape)
    lams = lam.reshape(LEVELS, HEADS, N_SEQ, TOK_DEV).transpose(2, 0, 1, 3)
    totals = jnp.einsum('nshi,nshj->nhij', ks.astype(jnp.float32), vs.astype(jnp.float32))
    masks = bucket_masks(N_SEQ, DEV_BITS)
    states = jnp.einsum('bnm,mhij->nbhij', masks, totals, precision=lax.Precision.HIGHEST).astype(jnp.bfloat16)
    attended = lax.map(lambda x: span_forward(*x)[0], (qs, ks, vs, lams, states))
    attended = attended.reshape(TOKENS, WIDTH)
    out = jnp.dot(attended, proj, preferred_element_type=jnp.float32).astype(jnp.bfloat16)
    grad_att = lax.dot_general(grad_out, proj, (((1,), (1,)), ((), ())), preferred_element_type=jnp.float32).astype(jnp.bfloat16)
    grad_proj = lax.dot_general(attended, grad_out, (((0,), (0,)), ((), ())), preferred_element_type=jnp.float32)
    dq, dk, dv, dlam, updates = lax.map(lambda x: span_backward(*x), (qs, ks, vs, lams, states, grad_att.reshape(shape)))
    returned = jnp.einsum('bnm,nbhij->mhij', masks, updates, precision=lax.Precision.HIGHEST).astype(jnp.bfloat16)
    dk = dk + jnp.einsum('nshj,nhij->nshi', vs.astype(jnp.float32), returned.astype(jnp.float32))
    dv = dv + jnp.einsum('nshi,nhij->nshj', ks.astype(jnp.float32), returned.astype(jnp.float32))
    dlam = dlam.transpose(1, 2, 0, 3).reshape(LEVELS, HEADS, TOKENS)
    return (out, dq.astype(jnp.bfloat16).reshape(TOKENS, WIDTH), dk.astype(jnp.bfloat16).reshape(TOKENS, WIDTH),
            dv.astype(jnp.bfloat16).reshape(TOKENS, WIDTH), dlam, grad_proj)


def reference(queries, keys, values, level_weights, proj, out_grad):
    out, dq, dk, dv, dlam, pieces = lax.map(lambda x: one_sequence(x[0], x[1], x[2], x[3], x[4], proj),
                                            (queries, keys, values, level_weights, out_grad))
    return out, dq, dk, dv, dlam, jnp.sum(pieces, axis=0)
```

```python
import functools

import jax
import jax.numpy as jnp
from jax import lax
from jax.experimental import pallas as pl
from jax.experimental.pallas import tpu as pltpu
from jax.sharding import PartitionSpec as P

BF16 = jnp.bfloat16
F32 = jnp.float32
LANES = 128


def flip(value, mask, axis="seq"):
    pairs = [(source, source ^ mask) for source in range(lax.axis_size(axis))]
    return lax.ppermute(value, axis, pairs)


def shift(value, step, axis="dp"):
    count = lax.axis_size(axis)
    pairs = [(source, (source + step) % count) for source in range(count)]
    return lax.ppermute(value, axis, pairs)


def dot_nn(a, b):
    return lax.dot_general(a, b, (((1,), (0,)), ((), ())), preferred_element_type=F32)


def dot_nt(a, b):
    return lax.dot_general(a, b, (((1,), (1,)), ((), ())), preferred_element_type=F32)


def dot_tn(a, b):
    return lax.dot_general(a, b, (((0,), (0,)), ((), ())), preferred_element_type=F32)


def call(body, outs, args, flops, name, scalars=0):
    vmem = pl.BlockSpec(memory_space=pltpu.VMEM)
    smem = pl.BlockSpec(memory_space=pltpu.SMEM)
    moved = sum(a.size * a.dtype.itemsize for a in args) + sum(
        jnp.dtype(d).itemsize * functools.reduce(lambda x, y: x * y, s, 1) for s, d in outs
    )
    return pl.pallas_call(
        body,
        out_shape=[jax.ShapeDtypeStruct(s, d) for s, d in outs],
        in_specs=[smem] * scalars + [vmem] * (len(args) - scalars),
        out_specs=[vmem] * len(outs),
        compiler_params=pltpu.CompilerParams(vmem_limit_bytes=24 * 1024 * 1024),
        cost_estimate=pl.CostEstimate(flops=int(flops), bytes_accessed=moved, transcendentals=0),
        name=name,
    )(*args)


class Dims:
    def __init__(self, queries, level_weights):
        self.tokens = queries.shape[1]
        self.width = queries.shape[2]
        self.levels = level_weights.shape[1]
        self.heads = level_weights.shape[2]
        self.size = self.width // self.heads
        self.scale = self.size ** (-0.5)
        self.bits = lax.axis_size("seq").bit_length() - 1
        self.local = self.levels - 1 - self.bits
        self.stretch = self.tokens >> self.local

    def head(self, h):
        return slice(h * self.size, (h + 1) * self.size)


def masks_st(d):
    s = lax.broadcasted_iota(jnp.int32, (d.tokens, d.tokens), 0)
    t = lax.broadcasted_iota(jnp.int32, (d.tokens, d.tokens), 1)
    apart = jnp.bitwise_xor(s // d.stretch, t // d.stretch)
    level = jnp.zeros((d.tokens, d.tokens), jnp.int32)
    for bit in range(d.local):
        level = level + (apart >= 1 << bit).astype(jnp.int32)
    return level, s <= t


def weights_st(d, lam_ref, h, level, causal):
    weight = jnp.broadcast_to(lam_ref[0, 0, h : h + 1, :], level.shape)
    for l in range(1, d.local + 1):
        weight = jnp.where(level == l, lam_ref[0, l, h : h + 1, :], weight)
    return jnp.where(causal, d.scale * weight, F32(0))


def totals_body(d, k_ref, v_ref, exact_ref, sent_ref):
    for h in range(d.heads):
        total = dot_tn(k_ref[0, :, d.head(h)], v_ref[0, :, d.head(h)])
        exact_ref[d.head(h), :] = total
        sent_ref[d.head(h), :] = total.astype(BF16)


def local_body(d, q_ref, k_ref, v_ref, lam_ref, total_ref, columns_ref):
    level, causal = masks_st(d)
    rows = [lam_ref[0, l] for l in range(d.levels)]
    rows.append(jnp.zeros((LANES - d.levels * d.heads, d.tokens), F32))
    columns_ref[...] = jnp.concatenate(rows, axis=0).T
    for h in range(d.heads):
        score = dot_nt(k_ref[0, :, d.head(h)], q_ref[0, :, d.head(h)])
        probs = (weights_st(d, lam_ref, h, level, causal) * score).astype(BF16)
        total_ref[:, d.head(h)] = dot_tn(probs, v_ref[0, :, d.head(h)])


def column(d, columns_ref, bit, h):
    at = (d.local + 1 + bit) * d.heads + h
    return columns_ref[:, at : at + 1]


def marked(place_ref, bit, value):
    keep = jnp.bitwise_and(jnp.right_shift(place_ref[0], bit), 1) > 0
    return jnp.where(keep, value, jnp.zeros_like(value))


def combine_body(d, place_ref, total_ref, q_ref, columns_ref, *refs):
    states, out_ref = refs[: d.bits], refs[d.bits]
    for h in range(d.heads):
        cross = jnp.zeros((d.tokens, d.size), F32)
        for bit in range(d.bits):
            state = marked(place_ref, bit, states[bit][d.head(h), :])
            cross = cross + column(d, columns_ref, bit, h) * dot_nn(q_ref[0, :, d.head(h)], state)
        out_ref[:, d.head(h)] = (total_ref[:, d.head(h)] + d.scale * cross).astype(BF16)


def updates_body(d, place_ref, q_ref, g_ref, columns_ref, *outs):
    for h in range(d.heads):
        g = g_ref[:, d.head(h)].astype(F32)
        for bit in range(d.bits):
            weighted = (d.scale * column(d, columns_ref, bit, h) * g).astype(BF16)
            update = dot_tn(q_ref[0, :, d.head(h)], weighted)
            outs[bit][d.head(h), :] = marked(place_ref, bit, update).astype(outs[bit].dtype)


def local_grads_body(d, place_ref, q_ref, k_ref, v_ref, g_ref, lam_ref, columns_ref, *refs):
    states = refs[: d.bits]
    gq_ref, dk_ref, dv_ref, gl_ref = refs[d.bits :]
    level, causal = masks_st(d)
    dots = []
    for h in range(d.heads):
        q, k, v = (r[0, :, d.head(h)] for r in (q_ref, k_ref, v_ref))
        g = g_ref[:, d.head(h)]
        gf = g.astype(F32)
        score = dot_nt(k, q)
        weight = weights_st(d, lam_ref, h, level, causal)
        probs = (weight * score).astype(BF16)
        dprob = dot_nt(v, g)
        dscore = (weight * dprob).astype(BF16)
        product = jnp.where(causal, d.scale * score * dprob, F32(0))
        for l in range(d.local + 1):
            part = jnp.where(level == l, product, F32(0))
            gl_ref[0, l, h : h + 1, :] = jnp.sum(part, axis=0, keepdims=True)
        gq = dot_tn(dscore, k)
        dk_ref[:, d.head(h)] = dot_nn(dscore, q)
        dv_ref[:, d.head(h)] = dot_nn(probs, g)
        for bit in range(d.bits):
            state = marked(place_ref, bit, states[bit][d.head(h), :])
            weighted = (d.scale * column(d, columns_ref, bit, h) * gf).astype(BF16)
            gq = gq + dot_nt(weighted, state)
            image = dot_nn(q, state)
            dots.append(d.scale * jnp.sum(gf * image, axis=1, keepdims=True))
        gq_ref[0, :, d.head(h)] = gq.astype(BF16)
    lane = lax.broadcasted_iota(jnp.int32, (d.tokens, LANES), 1)
    table = jnp.zeros((d.tokens, LANES), F32)
    for at, value in enumerate(dots):
        table = jnp.where(lane == at, value, table)
    rows = table.T
    for h in range(d.heads):
        for bit in range(d.bits):
            at = h * d.bits + bit
            gl_ref[0, d.local + 1 + bit, h : h + 1, :] = rows[at : at + 1, :]


def key_value_grads_body(d, k_ref, v_ref, dk_ref, dv_ref, back_ref, gk_ref, gv_ref):
    for h in range(d.heads):
        back = back_ref[d.head(h), :]
        gk = dk_ref[:, d.head(h)] + dot_nt(v_ref[0, :, d.head(h)], back)
        gv = dv_ref[:, d.head(h)] + dot_nn(k_ref[0, :, d.head(h)], back)
        gk_ref[0, :, d.head(h)] = gk.astype(BF16)
        gv_ref[0, :, d.head(h)] = gv.astype(BF16)


def block_columns(place_ref, mask, columns):
    owner = jnp.bitwise_xor(place_ref[0], mask)
    return pl.ds(pl.multiple_of(owner * columns, LANES), columns)


def grad_att_body(masks, columns, place_ref, og_ref, *refs):
    blocks, out_ref = refs[:-1], refs[-1]
    total = None
    for mask, block in zip(masks, blocks):
        part = dot_nt(og_ref[0, :, block_columns(place_ref, mask, columns)], block[...])
        total = part if total is None else total + part
    out_ref[...] = total.astype(BF16)


def project_body(masks, columns, place_ref, att_ref, *refs):
    blocks, out_ref = refs[:-1], refs[-1]
    for mask, block in zip(masks, blocks):
        out_ref[0, :, block_columns(place_ref, mask, columns)] = dot_nn(
            att_ref[...], block[...]
        ).astype(BF16)


def chip_sums_body(masks, columns, place_ref, att_ref, att2_ref, og_ref, og2_ref, *outs):
    first, second = att_ref[...].T, att2_ref[...].T
    for mask, out in zip(masks, outs):
        at = block_columns(place_ref, mask, columns)
        total = dot_nn(first, og_ref[0, :, at]) + dot_nn(second, og2_ref[0, :, at])
        out[...] = total.astype(out.dtype)


def chunks_body(count, place_ref, own_ref, *refs):
    arrived, mine_ref, outs = refs[: len(refs) - count], refs[-count], refs[len(refs) - count + 1 :]
    rows = mine_ref.shape[0]
    for step in range(count):
        owner = lax.rem(place_ref[0] + step, count)
        at = pl.ds(pl.multiple_of(owner * rows, 8), rows)
        total = own_ref[at, :]
        for block in arrived:
            total = total + block[at, :].astype(F32)
        if step == 0:
            mine_ref[...] = total
        else:
            outs[step - 1][...] = total.astype(BF16)


def chunk_sum_body(mine_ref, *refs):
    total = mine_ref[...]
    for block in refs[:-1]:
        total = total + block[...].astype(F32)
    refs[-1][...] = total.astype(BF16)


def assemble_body(count, place_ref, *refs):
    chunks, out_ref = refs[:-1], refs[-1]
    rows = chunks[0].shape[0]
    for step, chunk in enumerate(chunks):
        owner = lax.rem(place_ref[0] + count - step, count)
        out_ref[pl.ds(pl.multiple_of(owner * rows, 8), rows), :] = chunk[...].astype(F32)


def sum_over_dp(own, arrived):
    count = lax.axis_size("dp")
    rows, columns = own.shape[0] // count, own.shape[1]
    place = jnp.reshape(lax.axis_index("dp"), (1,)).astype(jnp.int32)
    mine, *send = call(
        functools.partial(chunks_body, count),
        [((rows, columns), F32)] + [((rows, columns), BF16)] * (count - 1),
        [place, own, *arrived],
        own.size * (1 + len(arrived)),
        "chunks",
        1,
    )
    got = [shift(value, step + 1) for step, value in enumerate(send)]
    (whole,) = call(
        chunk_sum_body, [((rows, columns), BF16)], [mine, *got], own.size, "chunk_sum"
    )
    spread = [whole] + [shift(whole, step) for step in range(1, count)]
    (out,) = call(
        functools.partial(assemble_body, count),
        [(own.shape, F32)],
        [place, *spread],
        own.size,
        "assemble",
        1,
    )
    return out


def shards(queries, keys, values, level_weights, proj, out_grad):
    d = Dims(queries, level_weights)
    devices = lax.axis_size("seq")
    columns = proj.shape[1]
    aligned = columns % LANES == 0
    place = jnp.reshape(lax.axis_index("seq"), (1,)).astype(jnp.int32)
    square = (d.width, d.size)
    flat = (d.tokens, d.width)
    mm = 2 * d.tokens * d.width

    exact, running = call(
        functools.partial(totals_body, d),
        [(square, F32), (square, BF16)],
        [keys, values],
        mm * d.size,
        "totals",
    )
    states = []
    for bit in range(d.bits):
        partner = flip(running, 1 << bit)
        states.append(partner)
        exact = exact + partner.astype(F32)
        running = exact.astype(BF16)

    chip = list(range(0, devices, 2))
    if aligned:
        mine = [proj] + [flip(proj, mask) for mask in chip[1:]]
        theirs = [flip(block, 1) for block in mine]
        og2 = flip(out_grad, 1)
        masks = chip + [mask + 1 for mask in chip]
        blocks = mine + theirs
    else:
        full = lax.all_gather(proj, "seq", axis=1, tiled=True)

    total, lam_columns = call(
        functools.partial(local_body, d),
        [(flat, F32), ((d.tokens, LANES), F32)],
        [queries, keys, values, level_weights],
        2 * mm * d.tokens,
        "local",
    )
    (attended,) = call(
        functools.partial(combine_body, d),
        [(flat, BF16)],
        [place, total, queries, lam_columns, *states],
        d.bits * mm * d.size,
        "combine",
        1,
    )
    if aligned:
        att2 = flip(attended, 1)
        own, *send = call(
            functools.partial(chip_sums_body, chip, columns),
            [((d.width, columns), F32)] + [((d.width, columns), BF16)] * (len(chip) - 1),
            [place, attended, att2, out_grad, og2],
            2 * mm * columns * len(chip),
            "chip_sums",
            1,
        )
        arrived = [flip(block, mask) for mask, block in zip(chip[1:], send)]
        (grad_att,) = call(
            functools.partial(grad_att_body, masks, columns),
            [(flat, BF16)],
            [place, out_grad, *blocks],
            mm * columns * devices,
            "grad_att",
            1,
        )
    else:
        grad_att = dot_nt(out_grad[0], full).astype(BF16)

    updates = call(
        functools.partial(updates_body, d),
        [(square, F32)] * (d.bits - 1) + [(square, BF16)],
        [place, queries, grad_att, lam_columns],
        d.bits * mm * d.size,
        "updates",
        1,
    )
    carried = None
    for bit in reversed(range(d.bits)):
        if carried is None:
            carried = flip(updates[bit], 1 << bit).astype(F32)
        else:
            carried = carried + flip((carried + updates[bit]).astype(BF16), 1 << bit).astype(F32)
    returned = carried.astype(BF16)

    grad_q, dk, dv, grad_levels = call(
        functools.partial(local_grads_body, d),
        [(queries.shape, BF16), (flat, F32), (flat, F32), (level_weights.shape, F32)],
        [place, queries, keys, values, grad_att, level_weights, lam_columns, *states],
        5 * mm * d.tokens + 2 * d.bits * mm * d.size,
        "local_grads",
        1,
    )
    grad_k, grad_v = call(
        functools.partial(key_value_grads_body, d),
        [(queries.shape, BF16), (queries.shape, BF16)],
        [keys, values, dk, dv, returned],
        2 * mm * d.size,
        "key_value_grads",
    )
    if aligned:
        (out,) = call(
            functools.partial(project_body, masks, columns),
            [(out_grad.shape, BF16)],
            [place, attended, *blocks],
            mm * columns * devices,
            "project",
            1,
        )
        grad_proj = sum_over_dp(own, arrived)
    else:
        out = dot_nn(attended, full).astype(BF16)[None]
        partial = dot_tn(out_grad[0], attended)
        shard = lax.psum_scatter(partial, "seq", scatter_dimension=0, tiled=True)
        grad_proj = lax.psum(shard, "dp").T
    return out, grad_q, grad_k, grad_v, grad_levels, grad_proj


def solution(mesh):
    rows = P("dp", "seq", None)
    return jax.shard_map(
        shards,
        mesh=mesh,
        in_specs=(rows, rows, rows, P("dp", None, None, "seq"), P(None, "seq"), rows),
        out_specs=(rows, rows, rows, rows, P("dp", None, None, "seq"), P(None, "seq")),
        check_vma=False,
    )
```
